32 devices in a mesh: fsdp: 4 (over x, core), ep: 8 (over z, y).
Axes of the slice: x: 2, y: 2, z: 4, core: 2. Of those that a mesh axis runs over, the one named last changes fastest.
Arguments:
- tokens: bfloat16 [256, 2048], P(('fsdp', 'ep')), may hold values from -6 to 6
- cotangent: bfloat16 [256, 2048], P(('fsdp', 'ep')), may hold values from -4 to 4
- routes: int32 [256, 2], P(('fsdp', 'ep')), may hold values from 0 to 7, as said below
- logits: float32 [256, 8], P(('fsdp', 'ep')), may hold values from -8 to 8
- w_gate: bfloat16 [2048, 16384], P('fsdp', 'ep'), may hold values from -0.125 to 0.125
- w_up: bfloat16 [2048, 16384], P('fsdp', 'ep'), may hold values from -0.125 to 0.125
- w_down: bfloat16 [16384, 2048], P('ep', 'fsdp'), may hold values from -0.0625 to 0.0625
Outputs:
- grad_tokens: bfloat16 [256, 2048], P(('fsdp', 'ep'))
- route_dot: float32 [256, 2], P(('fsdp', 'ep'))
- aux_grad: float32 [256, 8], P(('fsdp', 'ep'))
- grad_gate: bfloat16 [2048, 16384], P('fsdp', 'ep')
- grad_up: bfloat16 [2048, 16384], P('fsdp', 'ep')
- grad_down: bfloat16 [16384, 2048], P('ep', 'fsdp')
The draws below stay inside these ranges and needn't reach their ends.
Inputs may be any that keep to these rules, and one draw needn't show every extreme that they name: `routes`: each token names two different experts; on every device at most 3 tokens name one expert, and some expert is named by exactly 3 of them.
All inputs are finite; a program needn't handle non-finite values.
Results may differ from the reference program's by a relative error of at most 0.04.
Values may be sent and summed in bfloat16 or wider, within the bound.
A program may use at most 128 MiB of HBM per device.

```python
import jax
import jax.numpy as jnp
from jax import lax

D = 2048
FF = 8192
EXPERTS = 8
EXP_WIN = 2
TOK_DEV = 8
CAP = 3
TOKENS = 256
N_FSDP = 4
N_EP = 8


def draw_routes(key, part):
    nblocks = TOKENS // TOK_DEV
    rank = jnp.arange(nblocks, dtype=jnp.int32)
    jitter = jax.random.randint(jax.random.fold_in(key, 11), (nblocks,), 0, 3, dtype=jnp.int32)
    offset = rank * 6 // nblocks + jitter
    places = jnp.arange(TOK_DEV, dtype=jnp.int32)
    first = offset[:, None] + places[None, :] // CAP
    second = offset[:, None] + (places[None, :] + TOK_DEV) // CAP
    paired = jnp.stack([first, second], axis=2) % EXPERTS
    scores = jax.random.randint(jax.random.fold_in(key, 12), (nblocks, TOK_DEV), 0, 1 << 20, dtype=jnp.int32) * TOK_DEV + places[None, :]
    order = jnp.argsort(scores, axis=1, stable=True).astype(jnp.int32)
    paired = jnp.take_along_axis(paired, order[:, :, None], axis=1)
    flipped = jax.random.randint(jax.random.fold_in(key, 13), (nblocks, TOK_DEV, 1), 0, 2, dtype=jnp.int32)
    paired = jnp.where(flipped == 1, paired[:, :, ::-1], paired)
    return paired.reshape(TOKENS, 2).astype(jnp.int32)


def shard_levels(key, shape, pieces, least, high):
    def one(axis_at, parts):
        draws = jax.random.uniform(jax.random.fold_in(jax.random.fold_in(key, 6), axis_at), (parts,), jnp.float32, least / len(pieces), high / len(pieces))
        return jnp.repeat(jnp.exp(draws), shape[axis_at] // parts).reshape((-1,) + (1,) * (len(shape) - axis_at - 1))

    level = one(*pieces[0])
    for cut in pieces[1:]:
        level = level * one(*cut)
    return level


def bell_draw(key, dims, scale, bound, pieces=(), held_as=jnp.bfloat16):
    result = scale * jax.random.normal(key, dims, jnp.float32)
    if pieces:
        result = result * shard_levels(key, dims, pieces, -0.22, 0.18)
    return jnp.clip(result, -bound, bound).astype(held_as)


def setup_inputs(seed: int = 0) -> dict:
    splits = jax.random.split(jax.random.key(seed), 8)
    tokens = bell_draw(splits[0], (TOKENS, D), 1.0, 6.0, ((0, 32),))
    cotangent = bell_draw(splits[1], (TOKENS, D), 0.5, 4.0, ((0, 32),))
    routes = draw_routes(jax.random.fold_in(splits[7], 71), 0)
    logits = bell_draw(splits[3], (TOKENS, EXPERTS), 2.0, 8.0, ((0, 32),), jnp.float32)
    w_gate = bell_draw(splits[4], (D, EXP_WIN * FF), D ** -0.5, 0.125, ((0, 4), (1, 8)))
    w_up = bell_draw(splits[5], (D, EXP_WIN * FF), D ** -0.5, 0.125, ((0, 4), (1, 8)))
    w_down = bell_draw(splits[6], (EXP_WIN * FF, D), FF ** -0.5, 0.0625, ((0, 8), (1, 4)))
    return dict(tokens=tokens, cotangent=cotangent, routes=routes, logits=logits, w_gate=w_gate, w_up=w_up, w_down=w_down)


def routing(routes, logits):
    experts_all = logits.shape[-1]
    picked = (routes[:, :, None] == jnp.arange(experts_all, dtype=jnp.int32)[None, None, :]).astype(jnp.float32)
    chosen = jnp.sum(picked * logits[:, None, :], axis=2)
    combine = jax.nn.softmax(chosen, axis=1)
    window = picked[:, :, :EXP_WIN]
    member = jnp.sum(window, axis=1)
    scaled = jnp.sum(window * combine[:, :, None], axis=1)
    member_int = member.astype(jnp.int32)
    slot_ids = jnp.cumsum(member_int, axis=0) - member_int
    places = jnp.arange(CAP, dtype=jnp.int32)
    select = member[:, :, None] * (slot_ids[:, :, None] == places[None, None, :]).astype(jnp.float32)
    select = jnp.transpose(select, (1, 2, 0))
    slot_weight = jnp.einsum('xct,tx->xc', select, scaled)
    return select, slot_weight


def dispatch(select, slot_weight, tokens, cotangent):
    sent_tokens = jnp.einsum('xct,td->xcd', select, tokens.astype(jnp.float32)).astype(jnp.bfloat16)
    moved = jnp.einsum('xct,td->xcd', select, cotangent.astype(jnp.float32))
    sent_grads = (moved * slot_weight[:, :, None]).astype(jnp.bfloat16)
    return sent_tokens, sent_grads


def aux_gradient(routes, logits, total_counts):
    frac = total_counts.astype(jnp.float32) / jnp.sum(total_counts.astype(jnp.float32))
    probs = jax.nn.softmax(logits, axis=1)
    target = logits.shape[1] * frac
    return probs * (target[None, :] - jnp.sum(probs * target[None, :], axis=1, keepdims=True))


def expert_pass(rows_x, rows_dy, gate_w, up_w, down_w, blocks):
    gate_pre = jnp.dot(rows_x, gate_w, preferred_element_type=jnp.float32)
    up_pre = jnp.dot(rows_x, up_w, preferred_element_type=jnp.float32)
    sigma = jax.nn.sigmoid(gate_pre)
    active = gate_pre * sigma
    hidden = (active * up_pre).astype(jnp.bfloat16)
    hidden_grad = jnp.dot(rows_dy, down_w.T, preferred_element_type=jnp.float32)
    nrows = rows_x.shape[0]
    block_width = gate_w.shape[1] // blocks
    dots = jnp.sum((hidden.astype(jnp.float32) * hidden_grad).reshape(nrows, blocks, block_width), axis=2).astype(jnp.bfloat16)
    dots = jnp.sum(lax.optimization_barrier(dots).astype(jnp.float32), axis=1)
    up_grad = (hidden_grad * active).astype(jnp.bfloat16)
    gate_grad = (hidden_grad * up_pre * sigma * (1.0 + gate_pre * (1.0 - sigma))).astype(jnp.bfloat16)
    width_model = gate_w.shape[0]
    partial_value = jnp.einsum('rsf,dsf->srd', gate_grad.astype(jnp.float32).reshape(nrows, blocks, block_width),
                         gate_w.astype(jnp.float32).reshape(width_model, blocks, block_width))
    partial_value = partial_value + jnp.einsum('rsf,dsf->srd', up_grad.astype(jnp.float32).reshape(nrows, blocks, block_width),
                                   up_w.astype(jnp.float32).reshape(width_model, blocks, block_width))
    partial_value = lax.optimization_barrier(partial_value.astype(jnp.bfloat16))
    slot_grad = jnp.sum(partial_value.astype(jnp.float32), axis=0)
    grad_g = jnp.dot(rows_x.T, gate_grad, preferred_element_type=jnp.float32).astype(jnp.bfloat16)
    grad_u = jnp.dot(rows_x.T, up_grad, preferred_element_type=jnp.float32).astype(jnp.bfloat16)
    grad_d = jnp.dot(hidden.T, rows_dy, preferred_element_type=jnp.float32).astype(jnp.bfloat16)
    return slot_grad, dots, grad_g, grad_u, grad_d


def reference(tokens, cotangent, routes, logits, w_gate, w_up, w_down):
    blocks = N_EP // EXP_WIN
    tok = tokens.reshape(N_FSDP * N_EP, TOK_DEV, D)
    cot = cotangent.reshape(N_FSDP * N_EP, TOK_DEV, D)
    rts = routes.reshape(N_FSDP * N_EP, TOK_DEV, 2)
    lgt = logits.reshape(N_FSDP * N_EP, TOK_DEV, EXPERTS)
    select, slot_weight = jax.vmap(routing)(rts, lgt)
    sent_tokens, sent_grads = jax.vmap(dispatch)(select, slot_weight, tok, cot)
    sent_tokens = sent_tokens.reshape(N_FSDP, N_EP, EXP_WIN, CAP, D)
    sent_grads = sent_grads.reshape(N_FSDP, N_EP, EXP_WIN, CAP, D)

    def group_step(carry, blocks_in):
        acc_gate, acc_up, acc_down = carry
        group_x, group_dy = blocks_in
        grads_out = []
        dots_out = []
        for expert in range(EXP_WIN):
            low = expert * FF
            rows_x = group_x[:, expert].reshape(N_EP * CAP, D)
            rows_dy = group_dy[:, expert].reshape(N_EP * CAP, D)
            slot_grad, dots, grad_g, grad_u, grad_d = expert_pass(
                rows_x, rows_dy, w_gate[:, low:low + FF], w_up[:, low:low + FF], w_down[low:low + FF, :], blocks)
            acc_gate = acc_gate.at[:, low:low + FF].add(grad_g.astype(jnp.float32))
            acc_up = acc_up.at[:, low:low + FF].add(grad_u.astype(jnp.float32))
            acc_down = acc_down.at[low:low + FF, :].add(grad_d.astype(jnp.float32))
            grads_out.append(slot_grad.reshape(N_EP, CAP, D))
            dots_out.append(dots.reshape(N_EP, CAP))
        return (acc_gate, acc_up, acc_down), (jnp.stack(grads_out, axis=1), jnp.stack(dots_out, axis=1))

    start = (jnp.zeros((D, EXP_WIN * FF), jnp.float32), jnp.zeros((D, EXP_WIN * FF), jnp.float32),
             jnp.zeros((EXP_WIN * FF, D), jnp.float32))
    (acc_gate, acc_up, acc_down), (slot_grads, slot_dots) = lax.scan(group_step, start, (sent_tokens, sent_grads))
    slot_grads = slot_grads.reshape(N_FSDP * N_EP, EXP_WIN, CAP, D)
    slot_dots = slot_dots.reshape(N_FSDP * N_EP, EXP_WIN, CAP)
    grad_tokens = jnp.einsum('nxct,nxcd->ntd', select, slot_grads).reshape(TOKENS, D).astype(jnp.bfloat16)
    route_dot = jnp.einsum('nxct,nxc->ntx', select, slot_dots).reshape(TOKENS, EXP_WIN)
    total_counts = jnp.sum((routes[:, :, None] == jnp.arange(EXPERTS, dtype=jnp.int32)[None, None, :]).astype(jnp.int32), axis=(0, 1))
    aux_grad = aux_gradient(routes, logits, total_counts)
    return (grad_tokens, route_dot, aux_grad, acc_gate.astype(jnp.bfloat16), acc_up.astype(jnp.bfloat16),
            acc_down.astype(jnp.bfloat16))
```

```python
import functools

import jax
import jax.numpy as jnp
from jax import lax
from jax.experimental import pallas as pl
from jax.experimental.pallas import tpu as pltpu
from jax.sharding import PartitionSpec as P

EXP_WIN = 2
CAP = 3
PAD = 8
CORES = 2
CHUNKS = 4
LAST = (((1,), (1,)), ((), ()))
FIRST = (((0,), (0,)), ((), ()))
F32 = jnp.float32
BF16 = jnp.bfloat16
MESH = pl.DeviceIdType.MESH


def iota(shape, axis):
    return lax.broadcasted_iota(jnp.int32, shape, axis)


def kernel(
    n_fsdp, n_ep, chunks,
    tok_ref, cot_ref, routes_ref, logits_ref, wg_hbm, wu_hbm, wd_hbm,
    gt_ref, rd_ref, aux_ref, gg_hbm, gu_hbm, gd_hbm,
    wg, wu, wd, og, ou, od,
    send1, recv1, rows_x, rows_dy,
    own_a, send_a, recv_a, send_b, recv_b, acts, recv_c, dx, dots, send2, recv2,
    w_sem, o_sem, d_send, d_recv, a_send, a_recv, b_send, b_recv, c_send, c_recv, r_send, r_recv,
):
    n_dev = n_fsdp * n_ep
    n_x = n_fsdp // CORES
    blocks = n_ep // EXP_WIN
    f, e = lax.axis_index("fsdp"), lax.axis_index("ep")
    me = f * n_ep + e
    x, core = f // CORES, lax.rem(f, CORES)
    partner = x * CORES + (1 - core)
    depth, width = wg.shape
    half = width // CORES
    w = half // chunks

    barrier = pltpu.get_barrier_semaphore()

    def greet(j, _):
        d = lax.rem(me + j, n_dev)
        pl.semaphore_signal(barrier, inc=1, device_id=(d // n_ep, lax.rem(d, n_ep)), device_id_type=MESH)
        return 0

    lax.fori_loop(1, n_dev, greet, 0)
    loads = [
        pltpu.make_async_copy(s, t, w_sem.at[i])
        for i, (s, t) in enumerate(((wg_hbm, wg), (wu_hbm, wu), (wd_hbm, wd)))
    ]
    for c in loads:
        c.start()

    routes = routes_ref[...]
    logits = logits_ref[...]
    n_tok, n_exp = logits.shape
    r0, r1 = routes[:, 0:1], routes[:, 1:2]
    experts = iota((n_tok, n_exp), 1)
    c0 = jnp.sum(jnp.where(experts == r0, logits, 0.0), axis=1, keepdims=True)
    c1 = jnp.sum(jnp.where(experts == r1, logits, 0.0), axis=1, keepdims=True)
    top = jnp.maximum(c0, c1)
    e0, e1 = jnp.exp(c0 - top), jnp.exp(c1 - top)
    p0, p1 = e0 / (e0 + e1), e1 / (e0 + e1)
    ti, tj = iota((n_tok, n_tok), 0), iota((n_tok, n_tok), 1)
    ci = iota((PAD, n_tok), 0)
    lanes = iota((n_tok, depth), 1)
    counts = jnp.sum(
        jnp.where(lanes == r0, 1.0, 0.0) + jnp.where(lanes == r1, 1.0, 0.0), axis=0, keepdims=True
    )
    tok = tok_ref[...]
    cot = cot_ref[...].astype(F32)
    member_col, slot_col = [], []
    row_id = iota((PAD, depth), 0)
    for k in range(EXP_WIN):
        m0, m1 = jnp.where(r0 == k, 1.0, 0.0), jnp.where(r1 == k, 1.0, 0.0)
        col = m0 + m1
        weight = m0 * p0 + m1 * p1
        row = jnp.sum(jnp.where(ti == tj, col, 0.0), axis=0, keepdims=True)
        slot_row = jnp.sum(jnp.where(ti < tj, col, 0.0), axis=0, keepdims=True)
        slot_col.append(jnp.sum(jnp.where(tj < ti, row, 0.0), axis=1, keepdims=True))
        member_col.append(col)
        cf = ci.astype(F32)
        sel_a = jnp.where((cf == slot_row) & (ci < CAP), row, 0.0).astype(BF16)
        sel_b = jnp.where((cf - CAP == slot_row) & (ci < 2 * CAP), row, 0.0).astype(BF16)
        wcot = (cot * weight).astype(BF16)
        sent = jnp.dot(sel_a, tok, preferred_element_type=F32)
        sent = sent + jnp.dot(sel_b, wcot, preferred_element_type=F32)
        for g in range(n_fsdp):
            part = sent[:, g * depth : (g + 1) * depth]
            send1[k, g] = jnp.where(row_id == 2 * CAP, counts, part).astype(BF16)

    pl.semaphore_wait(barrier, n_dev - 1)

    def push(j, _):
        d = lax.rem(me + j, n_dev)
        df, de = d // n_ep, lax.rem(d, n_ep)
        pltpu.make_async_remote_copy(
            src_ref=send1.at[de // blocks, df], dst_ref=recv1.at[me], send_sem=d_send, recv_sem=d_recv,
            device_id=(df, de), device_id_type=MESH,
        ).start()
        return 0

    lax.fori_loop(1, n_dev, push, 0)
    recv1[me] = send1[e // blocks, f]
    everyone = recv1.at[pl.ds(0, n_dev - 1)]
    pltpu.make_async_copy(everyone, everyone, d_recv).wait()

    grp = min(32, n_dev)
    si, sj = iota((grp * CAP, grp * PAD), 0), iota((grp * CAP, grp * PAD), 1)
    base = (si // CAP) * PAD + lax.rem(si, CAP)
    pick_x = jnp.where(sj == base, 1.0, 0.0).astype(BF16)
    pick_dy = jnp.where(sj == base + CAP, 1.0, 0.0).astype(BF16)
    pick_c = jnp.where(
        lax.rem(iota((8, grp * PAD), 1), PAD) == 2 * CAP, 1.0, 0.0
    ).astype(BF16)
    total = jnp.zeros((8, depth), F32)
    for g in range(n_dev // grp):
        came = recv1[g * grp : (g + 1) * grp].reshape(grp * PAD, depth)
        span = pl.ds(g * grp * CAP, grp * CAP)
        rows_x[span] = jnp.dot(pick_x, came, preferred_element_type=F32).astype(BF16)
        rows_dy[span] = jnp.dot(pick_dy, came, preferred_element_type=F32).astype(BF16)
        total = total + jnp.dot(pick_c, came, preferred_element_type=F32)

    def copy_a(k):
        return pltpu.make_async_remote_copy(
            src_ref=send_a.at[k], dst_ref=recv_a.at[k], send_sem=a_send.at[k], recv_sem=a_recv.at[k],
            device_id=(partner, e), device_id_type=MESH,
        )

    def copy_b(k, j):
        to = lax.rem(x + j, n_x) * CORES + core
        return pltpu.make_async_remote_copy(
            src_ref=send_b.at[k], dst_ref=recv_b.at[k, j - 1], send_sem=b_send.at[k, j - 1],
            recv_sem=b_recv.at[k, j - 1], device_id=(to, e), device_id_type=MESH,
        )

    def copy_c(k):
        return pltpu.make_async_remote_copy(
            src_ref=acts.at[k], dst_ref=recv_c.at[k], send_sem=c_send.at[k], recv_sem=c_recv.at[k],
            device_id=(partner, e), device_id_type=MESH,
        )

    def columns(h, k):
        return pl.ds(pl.multiple_of(h * half + k * w, w), w)

    def partials(h, k):
        cols = columns(h, k)
        xs, dys = rows_x[...], rows_dy[...]
        yield jnp.dot(xs, wg[:, cols], preferred_element_type=F32)
        yield jnp.dot(xs, wu[:, cols], preferred_element_type=F32)
        yield lax.dot_general(dys, wd[cols, :], LAST, preferred_element_type=F32)

    def stage1(k):
        for i, v in enumerate(partials(1 - core, k)):
            send_a[k, i] = v.astype(BF16)
        copy_a(k).start()
        for i, v in enumerate(partials(core, k)):
            own_a[k, i] = v

    def stage2(k):
        copy_a(k).wait_recv()
        v = own_a[k] + recv_a[k].astype(F32)
        own_a[k] = v
        send_b[k] = v.astype(BF16)
        for j in range(1, n_x):
            copy_b(k, j).start()

    def stage3(k):
        for j in range(1, n_x):
            copy_b(k, j).wait_recv()
        pre = []
        for i in range(3):
            v = own_a[k, i]
            for j in range(n_x - 1):
                v = v + recv_b[k, j, i].astype(F32)
            pre.append(v)
        gate_pre, up_pre, hidden_grad = pre
        sigma = jax.nn.sigmoid(gate_pre)
        active = gate_pre * sigma
        hidden = (active * up_pre).astype(BF16)
        dot = jnp.sum(hidden.astype(F32) * hidden_grad, axis=1, keepdims=True)
        dots[...] = dot if k == 0 else dots[...] + dot
        acts[k, 0] = (hidden_grad * up_pre * sigma * (1.0 + gate_pre * (1.0 - sigma))).astype(BF16)
        acts[k, 1] = (hidden_grad * active).astype(BF16)
        acts[k, 2] = hidden
        copy_c(k).start()

    outs = ((og, gg_hbm), (ou, gu_hbm))

    def grads(h, k, source):
        cols = columns(h, k)
        xs, dys = rows_x[...], rows_dy[...]
        gate_grad, up_grad, hidden = source[k, 0], source[k, 1], source[k, 2]
        part = lax.dot_general(gate_grad, wg[:, cols], LAST, preferred_element_type=F32)
        part = part + lax.dot_general(up_grad, wu[:, cols], LAST, preferred_element_type=F32)
        og[:, cols] = lax.dot_general(xs, gate_grad, FIRST, preferred_element_type=F32).astype(BF16)
        ou[:, cols] = lax.dot_general(xs, up_grad, FIRST, preferred_element_type=F32).astype(BF16)
        od[cols, :] = lax.dot_general(hidden, dys, FIRST, preferred_element_type=F32).astype(BF16)
        return part

    def stores(h, k, slot):
        cols = columns(h, k)
        return [
            pltpu.make_async_copy(og.at[:, cols], gg_hbm.at[:, cols], o_sem.at[k, slot, 0]),
            pltpu.make_async_copy(ou.at[:, cols], gu_hbm.at[:, cols], o_sem.at[k, slot, 1]),
            pltpu.make_async_copy(od.at[cols, :], gd_hbm.at[cols, :], o_sem.at[k, slot, 2]),
        ]

    def stage4(k):
        part = grads(core, k, acts)
        for c in stores(core, k, 0):
            c.start()
        copy_c(k).wait_recv()
        part = part + grads(1 - core, k, recv_c)
        for c in stores(1 - core, k, 1):
            c.start()
        dx[...] = part if k == 0 else dx[...] + part

    for c in loads:
        c.wait()
    stage1(0)
    for k in range(1, chunks):
        stage1(k)
        stage2(k - 1)
    stage2(chunks - 1)

    count = total[0:1, 0:n_exp]
    target = n_exp * (count / jnp.sum(count, axis=1, keepdims=True))
    raised = jnp.exp(logits - jnp.max(logits, axis=1, keepdims=True))
    probs = raised / jnp.sum(raised, axis=1, keepdims=True)
    aux_ref[...] = probs * (target - jnp.sum(probs * target, axis=1, keepdims=True))

    stage3(0)
    for k in range(1, chunks):
        stage3(k)
        stage4(k - 1)
    stage4(chunks - 1)

    bi, bj = iota((grp * PAD, grp * CAP), 0), iota((grp * PAD, grp * CAP), 1)
    base = (bj // CAP) * PAD + lax.rem(bj, CAP)
    put_x = jnp.where(bi == base, 1.0, 0.0).astype(BF16)
    put_dot = jnp.where(bi == base + CAP, 1.0, 0.0).astype(BF16)
    once = jnp.where(x == 0, 1.0, 0.0)
    for g in range(n_dev // grp):
        span = pl.ds(g * grp * CAP, grp * CAP)
        mine = jnp.broadcast_to(dots[span] * once, (grp * CAP, depth)).astype(BF16)
        back = jnp.dot(put_x, dx[span].astype(BF16), preferred_element_type=F32)
        back = back + jnp.dot(put_dot, mine, preferred_element_type=F32)
        send2[g * grp : (g + 1) * grp] = back.astype(BF16).reshape(grp, PAD, depth)

    def give(j, _):
        d = lax.rem(me + j, n_dev)
        pltpu.make_async_remote_copy(
            src_ref=send2.at[d], dst_ref=recv2.at[me], send_sem=r_send, recv_sem=r_recv,
            device_id=(d // n_ep, lax.rem(d, n_ep)), device_id_type=MESH,
        ).start()
        return 0

    lax.fori_loop(1, n_dev, give, 0)
    recv2[me] = send2[me]
    everyone2 = recv2.at[pl.ds(0, n_dev - 1)]
    pltpu.make_async_copy(everyone2, everyone2, r_recv).wait()

    route = [jnp.zeros((1, 1), F32) for _ in range(EXP_WIN * CAP)]
    for g in range(n_fsdp):
        grad = jnp.zeros((n_tok, depth), F32)
        for k in range(EXP_WIN):
            acc = recv2[g * n_ep + k * blocks].astype(F32)
            for b in range(1, blocks):
                acc = acc + recv2[g * n_ep + k * blocks + b].astype(F32)
            for c in range(CAP):
                pick = jnp.where(slot_col[k] == c, member_col[k], 0.0)
                grad = grad + pick * acc[c : c + 1, :]
                route[k * CAP + c] = route[k * CAP + c] + acc[CAP + c : CAP + c + 1, 0:1]
        gt_ref[:, g * depth : (g + 1) * depth] = grad.astype(BF16)
    which = iota((n_tok, EXP_WIN), 1)
    out = jnp.zeros((n_tok, EXP_WIN), F32)
    for k in range(EXP_WIN):
        for c in range(CAP):
            pick = jnp.where(slot_col[k] == c, member_col[k], 0.0)
            out = out + jnp.where(which == k, pick * route[k * CAP + c], 0.0)
    rd_ref[...] = out

    pltpu.make_async_copy(everyone, everyone, d_send).wait()
    pltpu.make_async_copy(everyone2, everyone2, r_send).wait()
    for k in range(chunks):
        copy_a(k).wait_send()
        copy_c(k).wait_send()
        for j in range(1, n_x):
            copy_b(k, j).wait_send()
        for slot, h in enumerate((core, 1 - core)):
            for c in stores(h, k, slot):
                c.wait()


def body(n_fsdp, n_ep, tokens, cotangent, routes, logits, w_gate, w_up, w_down):
    n_tok, model = tokens.shape
    depth, width = w_gate.shape
    n_dev = n_fsdp * n_ep
    n_x = n_fsdp // CORES
    rows = n_dev * CAP
    half = width // CORES
    chunks = max(1, min(CHUNKS, half // 128))
    w = half // chunks
    vmem = pl.BlockSpec(memory_space=pltpu.VMEM)
    hbm = pl.BlockSpec(memory_space=pl.ANY)
    dma = pltpu.SemaphoreType.DMA
    return pl.pallas_call(
        functools.partial(kernel, n_fsdp, n_ep, chunks),
        out_shape=(
            jax.ShapeDtypeStruct((n_tok, model), BF16),
            jax.ShapeDtypeStruct((n_tok, EXP_WIN), F32),
            jax.ShapeDtypeStruct(logits.shape, F32),
            jax.ShapeDtypeStruct(w_gate.shape, BF16),
            jax.ShapeDtypeStruct(w_up.shape, BF16),
            jax.ShapeDtypeStruct(w_down.shape, BF16),
        ),
        in_specs=[vmem] * 4 + [hbm] * 3,
        out_specs=[vmem] * 3 + [hbm] * 3,
        scratch_shapes=[
            pltpu.VMEM(w_gate.shape, BF16),
            pltpu.VMEM(w_up.shape, BF16),
            pltpu.VMEM(w_down.shape, BF16),
            pltpu.VMEM(w_gate.shape, BF16),
            pltpu.VMEM(w_up.shape, BF16),
            pltpu.VMEM(w_down.shape, BF16),
            pltpu.VMEM((EXP_WIN, n_fsdp, PAD, depth), BF16),
            pltpu.VMEM((n_dev, PAD, depth), BF16),
            pltpu.VMEM((rows, depth), BF16),
            pltpu.VMEM((rows, depth), BF16),
            pltpu.VMEM((chunks, 3, rows, w), F32),
            pltpu.VMEM((chunks, 3, rows, w), BF16),
            pltpu.VMEM((chunks, 3, rows, w), BF16),
            pltpu.VMEM((chunks, 3, rows, w), BF16),
            pltpu.VMEM((chunks, n_x - 1, 3, rows, w), BF16),
            pltpu.VMEM((chunks, 3, rows, w), BF16),
            pltpu.VMEM((chunks, 3, rows, w), BF16),
            pltpu.VMEM((rows, depth), F32),
            pltpu.VMEM((rows, 1), F32),
            pltpu.VMEM((n_dev, PAD, depth), BF16),
            pltpu.VMEM((n_dev, PAD, depth), BF16),
            dma((3,)),
            dma((chunks, CORES, 3)),
            dma,
            dma,
            dma((chunks,)),
            dma((chunks,)),
            dma((chunks, n_x - 1)),
            dma((chunks, n_x - 1)),
            dma((chunks,)),
            dma((chunks,)),
            dma,
            dma,
        ],
        compiler_params=pltpu.CompilerParams(
            collective_id=0, has_side_effects=True, vmem_limit_bytes=62 * 1024 * 1024
        ),
    )(tokens, cotangent, routes, logits, w_gate, w_up, w_down)


def solution(mesh):
    in_specs = (
        P(("fsdp", "ep"), None),
        P(("fsdp", "ep"), None),
        P(("fsdp", "ep"), None),
        P(("fsdp", "ep"), None),
        P("fsdp", "ep"),
        P("fsdp", "ep"),
        P("ep", "fsdp"),
    )
    out_specs = (
        P(("fsdp", "ep"), None),
        P(("fsdp", "ep"), None),
        P(("fsdp", "ep"), None),
        P("fsdp", "ep"),
        P("fsdp", "ep"),
        P("ep", "fsdp"),
    )
    step = functools.partial(body, mesh.shape["fsdp"], mesh.shape["ep"])
    return jax.shard_map(step, mesh=mesh, in_specs=in_specs, out_specs=out_specs, check_vma=False)
```

```python
import functools

import jax
import jax.numpy as jnp
from jax import lax
from jax.experimental import pallas as pl
from jax.experimental.pallas import tpu as pltpu
from jax.sharding import PartitionSpec as P

EXP_WIN = 2
CAP = 3
PAD = 8
CORES = 2
CHUNKS = 4
LAST = (((1,), (1,)), ((), ()))
FIRST = (((0,), (0,)), ((), ()))
F32 = jnp.float32
BF16 = jnp.bfloat16
MESH = pl.DeviceIdType.MESH


def iota(shape, axis):
    return lax.broadcasted_iota(jnp.int32, shape, axis)


def kernel(
    n_fsdp, n_ep, chunks,
    tok_ref, cot_ref, routes_ref, logits_ref, wg_hbm, wu_hbm, wd_hbm,
    gt_ref, rd_ref, aux_ref, x_hbm, dy_hbm, acts_hbm,
    wg, wu, wd,
    send1, recv1, rows_x, rows_dy,
    own_a, send_a, recv_a, send_b, recv_b, acts, recv_c, dx, dots, send2, recv2,
    w_sem, o_sem, x_sem, d_send, d_recv, a_send, a_recv, b_send, b_recv, c_send, c_recv, r_send, r_recv,
):
    n_dev = n_fsdp * n_ep
    n_x = n_fsdp // CORES
    blocks = n_ep // EXP_WIN
    f, e = lax.axis_index("fsdp"), lax.axis_index("ep")
    me = f * n_ep + e
    x, core = f // CORES, lax.rem(f, CORES)
    partner = x * CORES + (1 - core)
    depth, width = wg.shape
    half = width // CORES
    w = half // chunks

    barrier = pltpu.get_barrier_semaphore()

    def greet(j, _):
        d = lax.rem(me + j, n_dev)
        pl.semaphore_signal(barrier, inc=1, device_id=(d // n_ep, lax.rem(d, n_ep)), device_id_type=MESH)
        return 0

    lax.fori_loop(1, n_dev, greet, 0)
    loads = [
        pltpu.make_async_copy(s, t, w_sem.at[i])
        for i, (s, t) in enumerate(((wg_hbm, wg), (wu_hbm, wu), (wd_hbm, wd)))
    ]
    for c in loads:
        c.start()

    routes = routes_ref[...]
    logits = logits_ref[...]
    n_tok, n_exp = logits.shape
    ti, tj = iota((n_tok, n_tok), 0), iota((n_tok, n_tok), 1)
    r0, r1 = (
        jnp.sum(jnp.where(ti == tj, routes[k : k + 1, :], 0), axis=1, keepdims=True) for k in range(2)
    )
    experts = iota((n_tok, n_exp), 1)
    c0 = jnp.sum(jnp.where(experts == r0, logits, 0.0), axis=1, keepdims=True)
    c1 = jnp.sum(jnp.where(experts == r1, logits, 0.0), axis=1, keepdims=True)
    top = jnp.maximum(c0, c1)
    e0, e1 = jnp.exp(c0 - top), jnp.exp(c1 - top)
    p0, p1 = e0 / (e0 + e1), e1 / (e0 + e1)
    ci = iota((PAD, n_tok), 0)
    lanes = iota((n_tok, depth), 1)
    counts = jnp.sum(
        jnp.where(lanes == r0, 1.0, 0.0) + jnp.where(lanes == r1, 1.0, 0.0), axis=0, keepdims=True
    )
    tok = tok_ref[...]
    cot = cot_ref[...].astype(F32)
    member_col, slot_col, member_row, slot_line = [], [], [], []
    row_id = iota((PAD, depth), 0)
    for k in range(EXP_WIN):
        m0, m1 = jnp.where(r0 == k, 1.0, 0.0), jnp.where(r1 == k, 1.0, 0.0)
        col = m0 + m1
        weight = m0 * p0 + m1 * p1
        row = jnp.sum(jnp.where(ti == tj, col, 0.0), axis=0, keepdims=True)
        slot_row = jnp.sum(jnp.where(ti < tj, col, 0.0), axis=0, keepdims=True)
        slot_col.append(jnp.sum(jnp.where(tj < ti, row, 0.0), axis=1, keepdims=True))
        member_col.append(col)
        member_row.append(row)
        slot_line.append(slot_row)
        cf = ci.astype(F32)
        sel_a = jnp.where((cf == slot_row) & (ci < CAP), row, 0.0).astype(BF16)
        sel_b = jnp.where((cf - CAP == slot_row) & (ci < 2 * CAP), row, 0.0).astype(BF16)
        wcot = (cot * weight).astype(BF16)
        sent = jnp.dot(sel_a, tok, preferred_element_type=F32)
        sent = sent + jnp.dot(sel_b, wcot, preferred_element_type=F32)
        for g in range(n_fsdp):
            part = sent[:, g * depth : (g + 1) * depth]
            send1[k, g] = jnp.where(row_id == 2 * CAP, counts, part).astype(BF16)

    pl.semaphore_wait(barrier, n_dev - 1)

    def push(j, _):
        d = lax.rem(me + j, n_dev)
        df, de = d // n_ep, lax.rem(d, n_ep)
        pltpu.make_async_remote_copy(
            src_ref=send1.at[de // blocks, df], dst_ref=recv1.at[me], send_sem=d_send, recv_sem=d_recv,
            device_id=(df, de), device_id_type=MESH,
        ).start()
        return 0

    lax.fori_loop(1, n_dev, push, 0)
    recv1[me] = send1[e // blocks, f]
    everyone = recv1.at[pl.ds(0, n_dev - 1)]
    pltpu.make_async_copy(everyone, everyone, d_recv).wait()

    grp = min(32, n_dev)
    si, sj = iota((grp * CAP, grp * PAD), 0), iota((grp * CAP, grp * PAD), 1)
    base = (si // CAP) * PAD + lax.rem(si, CAP)
    pick_x = jnp.where(sj == base, 1.0, 0.0).astype(BF16)
    pick_dy = jnp.where(sj == base + CAP, 1.0, 0.0).astype(BF16)
    pick_c = jnp.where(
        lax.rem(iota((8, grp * PAD), 1), PAD) == 2 * CAP, 1.0, 0.0
    ).astype(BF16)
    total = jnp.zeros((8, depth), F32)
    for g in range(n_dev // grp):
        came = recv1[g * grp : (g + 1) * grp].reshape(grp * PAD, depth)
        span = pl.ds(g * grp * CAP, grp * CAP)
        rows_x[span] = jnp.dot(pick_x, came, preferred_element_type=F32).astype(BF16)
        rows_dy[span] = jnp.dot(pick_dy, came, preferred_element_type=F32).astype(BF16)
        total = total + jnp.dot(pick_c, came, preferred_element_type=F32)

    def copy_a(k):
        return pltpu.make_async_remote_copy(
            src_ref=send_a.at[k], dst_ref=recv_a.at[k], send_sem=a_send.at[k], recv_sem=a_recv.at[k],
            device_id=(partner, e), device_id_type=MESH,
        )

    def copy_b(k, j):
        to = lax.rem(x + j, n_x) * CORES + core
        return pltpu.make_async_remote_copy(
            src_ref=send_b.at[k], dst_ref=recv_b.at[k, j - 1], send_sem=b_send.at[k, j - 1],
            recv_sem=b_recv.at[k, j - 1], device_id=(to, e), device_id_type=MESH,
        )

    def copy_c(k):
        return pltpu.make_async_remote_copy(
            src_ref=acts.at[k], dst_ref=recv_c.at[k], send_sem=c_send.at[k], recv_sem=c_recv.at[k],
            device_id=(partner, e), device_id_type=MESH,
        )

    def columns(h, k):
        return pl.ds(pl.multiple_of(h * half + k * w, w), w)

    def partials(h, k):
        cols = columns(h, k)
        xs, dys = rows_x[...], rows_dy[...]
        yield jnp.dot(xs, wg[:, cols], preferred_element_type=F32)
        yield jnp.dot(xs, wu[:, cols], preferred_element_type=F32)
        yield lax.dot_general(dys, wd[cols, :], LAST, preferred_element_type=F32)

    def stage1(k):
        for i, v in enumerate(partials(1 - core, k)):
            send_a[k, i] = v.astype(BF16)
        copy_a(k).start()
        for i, v in enumerate(partials(core, k)):
            own_a[k, i] = v

    def stage2(k):
        copy_a(k).wait_recv()
        v = own_a[k] + recv_a[k].astype(F32)
        own_a[k] = v
        send_b[k] = v.astype(BF16)
        for j in range(1, n_x):
            copy_b(k, j).start()

    def stage3(k):
        for j in range(1, n_x):
            copy_b(k, j).wait_recv()
        pre = []
        for i in range(3):
            v = own_a[k, i]
            for j in range(n_x - 1):
                v = v + recv_b[k, j, i].astype(F32)
            pre.append(v)
        gate_pre, up_pre, hidden_grad = pre
        sigma = jax.nn.sigmoid(gate_pre)
        active = gate_pre * sigma
        hidden = (active * up_pre).astype(BF16)
        dot = jnp.sum(hidden.astype(F32) * hidden_grad, axis=1, keepdims=True)
        dots[...] = dot if k == 0 else dots[...] + dot
        acts[k, 0] = (hidden_grad * up_pre * sigma * (1.0 + gate_pre * (1.0 - sigma))).astype(BF16)
        acts[k, 1] = (hidden_grad * active).astype(BF16)
        acts[k, 2] = hidden
        copy_c(k).start()

    def grads(h, k, source):
        cols = columns(h, k)
        part = lax.dot_general(source[k, 0], wg[:, cols], LAST, preferred_element_type=F32)
        return part + lax.dot_general(source[k, 1], wu[:, cols], LAST, preferred_element_type=F32)

    def store(h, k, slot, source):
        return pltpu.make_async_copy(source.at[k], acts_hbm.at[h, k], o_sem.at[k, slot])

    row_stores = [
        pltpu.make_async_copy(rows_x, x_hbm, x_sem.at[0]),
        pltpu.make_async_copy(rows_dy, dy_hbm, x_sem.at[1]),
    ]

    def stage4(k):
        part = grads(core, k, acts)
        store(core, k, 0, acts).start()
        copy_c(k).wait_recv()
        part = part + grads(1 - core, k, recv_c)
        store(1 - core, k, 1, recv_c).start()
        dx[...] = part if k == 0 else dx[...] + part

    for c in loads:
        c.wait()
    stage1(0)
    for k in range(1, chunks):
        stage1(k)
        stage2(k - 1)
    stage2(chunks - 1)

    for c in row_stores:
        c.start()

    count = total[0:1, 0:n_exp]
    target = n_exp * (count / jnp.sum(count, axis=1, keepdims=True))
    raised = jnp.exp(logits - jnp.max(logits, axis=1, keepdims=True))
    probs = raised / jnp.sum(raised, axis=1, keepdims=True)
    aux_ref[...] = probs * (target - jnp.sum(probs * target, axis=1, keepdims=True))

    stage3(0)
    for k in range(1, chunks):
        stage3(k)
        stage4(k - 1)
    stage4(chunks - 1)

    bi, bj = iota((grp * PAD, grp * CAP), 0), iota((grp * PAD, grp * CAP), 1)
    base = (bj // CAP) * PAD + lax.rem(bj, CAP)
    put_x = jnp.where(bi == base, 1.0, 0.0).astype(BF16)
    put_dot = jnp.where(bi == base + CAP, 1.0, 0.0).astype(BF16)
    once = jnp.where(x == 0, 1.0, 0.0)
    for g in range(n_dev // grp):
        span = pl.ds(g * grp * CAP, grp * CAP)
        mine = jnp.broadcast_to(dots[span] * once, (grp * CAP, depth)).astype(BF16)
        back = jnp.dot(put_x, dx[span].astype(BF16), preferred_element_type=F32)
        back = back + jnp.dot(put_dot, mine, preferred_element_type=F32)
        send2[g * grp : (g + 1) * grp] = back.astype(BF16).reshape(grp, PAD, depth)

    def give(j, _):
        d = lax.rem(me + j, n_dev)
        pltpu.make_async_remote_copy(
            src_ref=send2.at[d], dst_ref=recv2.at[me], send_sem=r_send, recv_sem=r_recv,
            device_id=(d // n_ep, lax.rem(d, n_ep)), device_id_type=MESH,
        ).start()
        return 0

    lax.fori_loop(1, n_dev, give, 0)
    recv2[me] = send2[me]
    everyone2 = recv2.at[pl.ds(0, n_dev - 1)]
    pltpu.make_async_copy(everyone2, everyone2, r_recv).wait()

    route = [jnp.zeros((1, 1), F32) for _ in range(EXP_WIN * CAP)]
    for g in range(n_fsdp):
        grad = jnp.zeros((n_tok, depth), F32)
        for k in range(EXP_WIN):
            acc = recv2[g * n_ep + k * blocks].astype(F32)
            for b in range(1, blocks):
                acc = acc + recv2[g * n_ep + k * blocks + b].astype(F32)
            for c in range(CAP):
                pick = jnp.where(slot_col[k] == c, member_col[k], 0.0)
                grad = grad + pick * acc[c : c + 1, :]
                route[k * CAP + c] = route[k * CAP + c] + acc[CAP + c : CAP + c + 1, 0:1]
        gt_ref[:, g * depth : (g + 1) * depth] = grad.astype(BF16)
    which = iota((EXP_WIN, n_tok), 0)
    out = jnp.zeros((EXP_WIN, n_tok), F32)
    for k in range(EXP_WIN):
        for c in range(CAP):
            pick = jnp.where(slot_line[k] == c, member_row[k], 0.0)
            out = out + jnp.where(which == k, pick * route[k * CAP + c], 0.0)
    rd_ref[...] = out

    pltpu.make_async_copy(everyone, everyone, d_send).wait()
    pltpu.make_async_copy(everyone2, everyone2, r_send).wait()
    for k in range(chunks):
        copy_a(k).wait_send()
        copy_c(k).wait_send()
        for j in range(1, n_x):
            copy_b(k, j).wait_send()
        store(core, k, 0, acts).wait()
        store(1 - core, k, 1, recv_c).wait()
    for c in row_stores:
        c.wait()


def weight_kernel(x_ref, dy_ref, acts_ref, gt_in, rd_in, aux_in, gt_ref, rd_ref, aux_ref, og, ou, od):
    xs, dys = x_ref[...], dy_ref[...]
    og[...] = lax.dot_general(xs, acts_ref[0], FIRST, preferred_element_type=F32).astype(BF16)
    ou[...] = lax.dot_general(xs, acts_ref[1], FIRST, preferred_element_type=F32).astype(BF16)
    od[...] = lax.dot_general(acts_ref[2], dys, FIRST, preferred_element_type=F32).astype(BF16)

    @pl.when(pl.program_id(0) == 0)
    def _():
        gt_ref[...] = gt_in[...]
        rd_ref[...] = rd_in[...]
        aux_ref[...] = aux_in[...]


def body(n_fsdp, n_ep, tokens, cotangent, routes, logits, w_gate, w_up, w_down):
    n_tok, model = tokens.shape
    depth, width = w_gate.shape
    n_dev = n_fsdp * n_ep
    n_x = n_fsdp // CORES
    rows = n_dev * CAP
    half = width // CORES
    chunks = max(1, min(CHUNKS, half // 128))
    w = half // chunks
    vmem = pl.BlockSpec(memory_space=pltpu.VMEM)
    hbm = pl.BlockSpec(memory_space=pl.ANY)
    dma = pltpu.SemaphoreType.DMA
    small_x, small_r, small_a, all_x, all_dy, all_acts = pl.pallas_call(
        functools.partial(kernel, n_fsdp, n_ep, chunks),
        out_shape=(
            jax.ShapeDtypeStruct((n_tok, model), BF16),
            jax.ShapeDtypeStruct((EXP_WIN, n_tok), F32),
            jax.ShapeDtypeStruct(logits.shape, F32),
            jax.ShapeDtypeStruct((rows, depth), BF16),
            jax.ShapeDtypeStruct((rows, depth), BF16),
            jax.ShapeDtypeStruct((CORES, chunks, 3, rows, w), BF16),
        ),
        in_specs=[vmem] * 4 + [hbm] * 3,
        out_specs=[vmem] * 3 + [hbm] * 3,
        scratch_shapes=[
            pltpu.VMEM(w_gate.shape, BF16),
            pltpu.VMEM(w_up.shape, BF16),
            pltpu.VMEM(w_down.shape, BF16),
            pltpu.VMEM((EXP_WIN, n_fsdp, PAD, depth), BF16),
            pltpu.VMEM((n_dev, PAD, depth), BF16),
            pltpu.VMEM((rows, depth), BF16),
            pltpu.VMEM((rows, depth), BF16),
            pltpu.VMEM((chunks, 3, rows, w), F32),
            pltpu.VMEM((chunks, 3, rows, w), BF16),
            pltpu.VMEM((chunks, 3, rows, w), BF16),
            pltpu.VMEM((chunks, 3, rows, w), BF16),
            pltpu.VMEM((chunks, n_x - 1, 3, rows, w), BF16),
            pltpu.VMEM((chunks, 3, rows, w), BF16),
            pltpu.VMEM((chunks, 3, rows, w), BF16),
            pltpu.VMEM((rows, depth), F32),
            pltpu.VMEM((rows, 1), F32),
            pltpu.VMEM((n_dev, PAD, depth), BF16),
            pltpu.VMEM((n_dev, PAD, depth), BF16),
            dma((3,)),
            dma((chunks, CORES)),
            dma((2,)),
            dma,
            dma,
            dma((chunks,)),
            dma((chunks,)),
            dma((chunks, n_x - 1)),
            dma((chunks, n_x - 1)),
            dma((chunks,)),
            dma((chunks,)),
            dma,
            dma,
        ],
        compiler_params=pltpu.CompilerParams(
            collective_id=0, has_side_effects=True, vmem_limit_bytes=62 * 1024 * 1024
        ),
    )(tokens, cotangent, jnp.transpose(routes), logits, w_gate, w_up, w_down)
    step = min(256, w)
    per = w // step

    def same(i):
        return (0, 0)

    def whole(a):
        return pl.BlockSpec(a.shape, same)

    smalls = [whole(small_x), whole(small_r), whole(small_a)]
    cols = pl.BlockSpec((depth, step), lambda i: (0, i))
    out = pl.pallas_call(
        weight_kernel,
        grid=(width // step,),
        out_shape=(
            jax.ShapeDtypeStruct(small_x.shape, BF16),
            jax.ShapeDtypeStruct(small_r.shape, F32),
            jax.ShapeDtypeStruct(small_a.shape, F32),
            jax.ShapeDtypeStruct(w_gate.shape, BF16),
            jax.ShapeDtypeStruct(w_up.shape, BF16),
            jax.ShapeDtypeStruct(w_down.shape, BF16),
        ),
        in_specs=[
            whole(all_x),
            whole(all_dy),
            pl.BlockSpec(
                (None, None, 3, rows, step),
                lambda i: (i // (chunks * per), lax.rem(i // per, chunks), 0, 0, lax.rem(i, per)),
            ),
        ]
        + smalls,
        out_specs=smalls + [cols, cols, pl.BlockSpec((step, depth), lambda i: (i, 0))],
        compiler_params=pltpu.CompilerParams(dimension_semantics=("arbitrary",)),
    )(all_x, all_dy, all_acts, small_x, small_r, small_a)
    return (out[0], jnp.transpose(out[1])) + tuple(out[2:])


def solution(mesh):
    in_specs = (
        P(("fsdp", "ep"), None),
        P(("fsdp", "ep"), None),
        P(("fsdp", "ep"), None),
        P(("fsdp", "ep"), None),
        P("fsdp", "ep"),
        P("fsdp", "ep"),
        P("ep", "fsdp"),
    )
    out_specs = (
        P(("fsdp", "ep"), None),
        P(("fsdp", "ep"), None),
        P(("fsdp", "ep"), None),
        P("fsdp", "ep"),
        P("fsdp", "ep"),
        P("ep", "fsdp"),
    )
    step = functools.partial(body, mesh.shape["fsdp"], mesh.shape["ep"])
    return jax.shard_map(step, mesh=mesh, in_specs=in_specs, out_specs=out_specs, check_vma=False)
```

```python
import functools

import jax
import jax.numpy as jnp
from jax import lax
from jax.experimental import pallas as pl
from jax.experimental.pallas import tpu as pltpu
from jax.sharding import PartitionSpec as P

EXP_WIN = 2
CAP = 3
PAD = 8
CORES = 2
CHUNKS = 4
GROUPS = 2
LAST = (((1,), (1,)), ((), ()))
FIRST = (((0,), (0,)), ((), ()))
F32 = jnp.float32
BF16 = jnp.bfloat16
MESH = pl.DeviceIdType.MESH


def iota(shape, axis):
    return lax.broadcasted_iota(jnp.int32, shape, axis)


def kernel(
    n_fsdp, n_ep, chunks,
    tok_ref, cot_ref, routes_ref, logits_ref, wg_hbm, wu_hbm, wd_hbm,
    gt_ref, rd_ref, aux_ref, x_hbm, dy_hbm, acts_hbm,
    wg, wu, wd,
    send1, recv1, rows_x, rows_dy,
    own_a, send_a, recv_a, send_b, recv_b, acts, recv_c, dx, dots, send2, recv2,
    w_sem, o_sem, x_sem, d_send, d_recv, a_send, a_recv, b_send, b_recv, c_send, c_recv, r_send, r_recv,
):
    n_dev = n_fsdp * n_ep
    n_x = n_fsdp // CORES
    blocks = n_ep // EXP_WIN
    f, e = lax.axis_index("fsdp"), lax.axis_index("ep")
    me = f * n_ep + e
    x, core = f // CORES, lax.rem(f, CORES)
    partner = x * CORES + (1 - core)
    depth, width = wg.shape
    half = width // CORES
    w = half // chunks
    ring = n_ep // GROUPS
    size = n_fsdp * ring
    span_rows = size * CAP
    place = f * ring + e // GROUPS

    def peer(t, i):
        return i // ring, lax.rem(i, ring) * GROUPS + lax.rem(e + t, GROUPS)

    barrier = pltpu.get_barrier_semaphore()

    def greet(j, _):
        d = lax.rem(me + j, n_dev)
        pl.semaphore_signal(barrier, inc=1, device_id=(d // n_ep, lax.rem(d, n_ep)), device_id_type=MESH)
        return 0

    lax.fori_loop(1, n_dev, greet, 0)
    loads = [
        pltpu.make_async_copy(s, t, w_sem.at[i])
        for i, (s, t) in enumerate(((wg_hbm, wg), (wu_hbm, wu), (wd_hbm, wd)))
    ]
    for c in loads:
        c.start()

    routes = routes_ref[...]
    logits = logits_ref[...]
    n_tok, n_exp = logits.shape
    ti, tj = iota((n_tok, n_tok), 0), iota((n_tok, n_tok), 1)
    r0, r1 = (
        jnp.sum(jnp.where(ti == tj, routes[k : k + 1, :], 0), axis=1, keepdims=True) for k in range(2)
    )
    experts = iota((n_tok, n_exp), 1)
    c0 = jnp.sum(jnp.where(experts == r0, logits, 0.0), axis=1, keepdims=True)
    c1 = jnp.sum(jnp.where(experts == r1, logits, 0.0), axis=1, keepdims=True)
    top = jnp.maximum(c0, c1)
    e0, e1 = jnp.exp(c0 - top), jnp.exp(c1 - top)
    p0, p1 = e0 / (e0 + e1), e1 / (e0 + e1)
    ci = iota((PAD, n_tok), 0)
    lanes = iota((n_tok, depth), 1)
    counts = jnp.sum(
        jnp.where(lanes == r0, 1.0, 0.0) + jnp.where(lanes == r1, 1.0, 0.0), axis=0, keepdims=True
    )
    tok = tok_ref[...]
    cot = cot_ref[...].astype(F32)
    member_col, slot_col, member_row, slot_line = [], [], [], []
    row_id = iota((PAD, depth), 0)
    for k in range(EXP_WIN):
        m0, m1 = jnp.where(r0 == k, 1.0, 0.0), jnp.where(r1 == k, 1.0, 0.0)
        col = m0 + m1
        weight = m0 * p0 + m1 * p1
        row = jnp.sum(jnp.where(ti == tj, col, 0.0), axis=0, keepdims=True)
        slot_row = jnp.sum(jnp.where(ti < tj, col, 0.0), axis=0, keepdims=True)
        slot_col.append(jnp.sum(jnp.where(tj < ti, row, 0.0), axis=1, keepdims=True))
        member_col.append(col)
        member_row.append(row)
        slot_line.append(slot_row)
        cf = ci.astype(F32)
        sel_a = jnp.where((cf == slot_row) & (ci < CAP), row, 0.0).astype(BF16)
        sel_b = jnp.where((cf - CAP == slot_row) & (ci < 2 * CAP), row, 0.0).astype(BF16)
        wcot = (cot * weight).astype(BF16)
        sent = jnp.dot(sel_a, tok, preferred_element_type=F32)
        sent = sent + jnp.dot(sel_b, wcot, preferred_element_type=F32)
        for g in range(n_fsdp):
            part = sent[:, g * depth : (g + 1) * depth]
            send1[k, g] = jnp.where(row_id == 2 * CAP, counts, part).astype(BF16)

    pl.semaphore_wait(barrier, n_dev - 1)

    recv1[place] = send1[e // blocks, f]
    for t in range(GROUPS):
        back_t = (GROUPS - t) % GROUPS

        def push(j, _, t=t, back_t=back_t):
            df, de = peer(t, lax.rem(place + j, size))
            pltpu.make_async_remote_copy(
                src_ref=send1.at[de // blocks, df], dst_ref=recv1.at[back_t * size + place],
                send_sem=d_send, recv_sem=d_recv.at[back_t], device_id=(df, de), device_id_type=MESH,
            ).start()
            return 0

        lax.fori_loop(1 if t == 0 else 0, size, push, 0)

    grp = min(16, size)
    si, sj = iota((grp * CAP, grp * PAD), 0), iota((grp * CAP, grp * PAD), 1)
    base = (si // CAP) * PAD + lax.rem(si, CAP)
    pick_x = jnp.where(sj == base, 1.0, 0.0).astype(BF16)
    pick_dy = jnp.where(sj == base + CAP, 1.0, 0.0).astype(BF16)
    pick_c = jnp.where(
        lax.rem(iota((8, grp * PAD), 1), PAD) == 2 * CAP, 1.0, 0.0
    ).astype(BF16)

    def prepare(t, total):
        landed = recv1.at[pl.ds(t * size, size - 1 if t == 0 else size)]
        pltpu.make_async_copy(landed, landed, d_recv.at[t]).wait()
        for g in range(t * size // grp, (t + 1) * size // grp):
            came = recv1[g * grp : (g + 1) * grp].reshape(grp * PAD, depth)
            span = pl.ds(g * grp * CAP, grp * CAP)
            rows_x[span] = jnp.dot(pick_x, came, preferred_element_type=F32).astype(BF16)
            rows_dy[span] = jnp.dot(pick_dy, came, preferred_element_type=F32).astype(BF16)
            total = total + jnp.dot(pick_c, came, preferred_element_type=F32)
        return total

    def copy_a(k):
        return pltpu.make_async_remote_copy(
            src_ref=send_a.at[k], dst_ref=recv_a.at[k], send_sem=a_send.at[k], recv_sem=a_recv.at[k],
            device_id=(partner, e), device_id_type=MESH,
        )

    def copy_b(k, j):
        to = lax.rem(x + j, n_x) * CORES + core
        return pltpu.make_async_remote_copy(
            src_ref=send_b.at[k], dst_ref=recv_b.at[k, j - 1], send_sem=b_send.at[k, j - 1],
            recv_sem=b_recv.at[k, j - 1], device_id=(to, e), device_id_type=MESH,
        )

    def copy_c(k):
        return pltpu.make_async_remote_copy(
            src_ref=acts.at[k], dst_ref=recv_c.at[k], send_sem=c_send.at[k], recv_sem=c_recv.at[k],
            device_id=(partner, e), device_id_type=MESH,
        )

    def columns(h, k):
        return pl.ds(pl.multiple_of(h * half + k * w, w), w)

    def group(u):
        return pl.ds(u // chunks * span_rows, span_rows)

    def partials(h, u):
        cols = columns(h, u % chunks)
        xs, dys = rows_x[group(u)], rows_dy[group(u)]
        yield jnp.dot(xs, wg[:, cols], preferred_element_type=F32)
        yield jnp.dot(xs, wu[:, cols], preferred_element_type=F32)
        yield lax.dot_general(dys, wd[cols, :], LAST, preferred_element_type=F32)

    def stage1(k):
        for i, v in enumerate(partials(1 - core, k)):
            send_a[k, i] = v.astype(BF16)
        copy_a(k).start()
        for i, v in enumerate(partials(core, k)):
            own_a[k, i] = v

    def stage2(k):
        copy_a(k).wait_recv()
        v = own_a[k] + recv_a[k].astype(F32)
        own_a[k] = v
        send_b[k] = v.astype(BF16)
        for j in range(1, n_x):
            copy_b(k, j).start()

    def stage3(k):
        for j in range(1, n_x):
            copy_b(k, j).wait_recv()
        pre = []
        for i in range(3):
            v = own_a[k, i]
            for j in range(n_x - 1):
                v = v + recv_b[k, j, i].astype(F32)
            pre.append(v)
        gate_pre, up_pre, hidden_grad = pre
        sigma = jax.nn.sigmoid(gate_pre)
        active = gate_pre * sigma
        hidden = (active * up_pre).astype(BF16)
        dot = jnp.sum(hidden.astype(F32) * hidden_grad, axis=1, keepdims=True)
        dots[group(k)] = dot if k % chunks == 0 else dots[group(k)] + dot
        acts[k, 0] = (hidden_grad * up_pre * sigma * (1.0 + gate_pre * (1.0 - sigma))).astype(BF16)
        acts[k, 1] = (hidden_grad * active).astype(BF16)
        acts[k, 2] = hidden
        copy_c(k).start()

    def grads(h, k, source):
        cols = columns(h, k % chunks)
        part = lax.dot_general(source[k, 0], wg[:, cols], LAST, preferred_element_type=F32)
        return part + lax.dot_general(source[k, 1], wu[:, cols], LAST, preferred_element_type=F32)

    def store(h, k, slot, source):
        return pltpu.make_async_copy(source.at[k], acts_hbm.at[h, k % chunks, :, group(k), :], o_sem.at[k, slot])

    row_stores = [
        pltpu.make_async_copy(rows_x, x_hbm, x_sem.at[0]),
        pltpu.make_async_copy(rows_dy, dy_hbm, x_sem.at[1]),
    ]

    def stage4(k):
        part = grads(core, k, acts)
        store(core, k, 0, acts).start()
        copy_c(k).wait_recv()
        part = part + grads(1 - core, k, recv_c)
        store(1 - core, k, 1, recv_c).start()
        dx[group(k)] = part if k % chunks == 0 else dx[group(k)] + part

    for c in loads:
        c.wait()
    total = jnp.zeros((8, depth), F32)
    for t in range(GROUPS):
        total = prepare(t, total)
        for k in range(t * chunks, (t + 1) * chunks):
            stage1(k)
            if k > 0:
                stage2(k - 1)
    stage2(GROUPS * chunks - 1)

    for c in row_stores:
        c.start()

    count = total[0:1, 0:n_exp]
    target = n_exp * (count / jnp.sum(count, axis=1, keepdims=True))
    raised = jnp.exp(logits - jnp.max(logits, axis=1, keepdims=True))
    probs = raised / jnp.sum(raised, axis=1, keepdims=True)
    aux_ref[...] = probs * (target - jnp.sum(probs * target, axis=1, keepdims=True))

    bi, bj = iota((grp * PAD, grp * CAP), 0), iota((grp * PAD, grp * CAP), 1)
    base = (bj // CAP) * PAD + lax.rem(bj, CAP)
    put_x = jnp.where(bi == base, 1.0, 0.0).astype(BF16)
    put_dot = jnp.where(bi == base + CAP, 1.0, 0.0).astype(BF16)
    once = jnp.where(x == 0, 1.0, 0.0)

    def give_back(t):
        for g in range(t * size // grp, (t + 1) * size // grp):
            span = pl.ds(g * grp * CAP, grp * CAP)
            mine = jnp.broadcast_to(dots[span] * once, (grp * CAP, depth)).astype(BF16)
            back = jnp.dot(put_x, dx[span].astype(BF16), preferred_element_type=F32)
            back = back + jnp.dot(put_dot, mine, preferred_element_type=F32)
            send2[g * grp : (g + 1) * grp] = back.astype(BF16).reshape(grp, PAD, depth)

        def give(j, _):
            i = lax.rem(place + j, size)
            pltpu.make_async_remote_copy(
                src_ref=send2.at[t * size + i], dst_ref=recv2.at[me], send_sem=r_send, recv_sem=r_recv,
                device_id=peer(t, i), device_id_type=MESH,
            ).start()
            return 0

        lax.fori_loop(1 if t == 0 else 0, size, give, 0)
        if t == 0:
            recv2[me] = send2[place]

    for k in range(GROUPS * chunks):
        stage3(k)
        if k > 0:
            stage4(k - 1)
            if k % chunks == 0:
                give_back(k // chunks - 1)
    stage4(GROUPS * chunks - 1)
    give_back(GROUPS - 1)
    everyone = recv1.at[pl.ds(0, n_dev - 1)]
    everyone2 = recv2.at[pl.ds(0, n_dev - 1)]
    pltpu.make_async_copy(everyone2, everyone2, r_recv).wait()

    route = [jnp.zeros((1, 1), F32) for _ in range(EXP_WIN * CAP)]
    for g in range(n_fsdp):
        grad = jnp.zeros((n_tok, depth), F32)
        for k in range(EXP_WIN):
            acc = recv2[g * n_ep + k * blocks].astype(F32)
            for b in range(1, blocks):
                acc = acc + recv2[g * n_ep + k * blocks + b].astype(F32)
            for c in range(CAP):
                pick = jnp.where(slot_col[k] == c, member_col[k], 0.0)
                grad = grad + pick * acc[c : c + 1, :]
                route[k * CAP + c] = route[k * CAP + c] + acc[CAP + c : CAP + c + 1, 0:1]
        gt_ref[:, g * depth : (g + 1) * depth] = grad.astype(BF16)
    which = iota((EXP_WIN, n_tok), 0)
    out = jnp.zeros((EXP_WIN, n_tok), F32)
    for k in range(EXP_WIN):
        for c in range(CAP):
            pick = jnp.where(slot_line[k] == c, member_row[k], 0.0)
            out = out + jnp.where(which == k, pick * route[k * CAP + c], 0.0)
    rd_ref[...] = out

    pltpu.make_async_copy(everyone, everyone, d_send).wait()
    pltpu.make_async_copy(everyone2, everyone2, r_send).wait()
    for k in range(GROUPS * chunks):
        copy_a(k).wait_send()
        copy_c(k).wait_send()
        for j in range(1, n_x):
            copy_b(k, j).wait_send()
        store(core, k, 0, acts).wait()
        store(1 - core, k, 1, recv_c).wait()
    for c in row_stores:
        c.wait()


def weight_kernel(x_ref, dy_ref, acts_ref, gt_in, rd_in, aux_in, gt_ref, rd_ref, aux_ref, og, ou, od):
    xs, dys = x_ref[...], dy_ref[...]
    og[...] = lax.dot_general(xs, acts_ref[0], FIRST, preferred_element_type=F32).astype(BF16)
    ou[...] = lax.dot_general(xs, acts_ref[1], FIRST, preferred_element_type=F32).astype(BF16)
    od[...] = lax.dot_general(acts_ref[2], dys, FIRST, preferred_element_type=F32).astype(BF16)

    @pl.when(pl.program_id(0) == 0)
    def _():
        gt_ref[...] = gt_in[...]
        rd_ref[...] = rd_in[...]
        aux_ref[...] = aux_in[...]


def body(n_fsdp, n_ep, tokens, cotangent, routes, logits, w_gate, w_up, w_down):
    n_tok, model = tokens.shape
    depth, width = w_gate.shape
    n_dev = n_fsdp * n_ep
    n_x = n_fsdp // CORES
    rows = n_dev * CAP
    half = width // CORES
    chunks = max(1, min(CHUNKS, half // 128))
    w = half // chunks
    items, part = GROUPS * chunks, rows // GROUPS
    vmem = pl.BlockSpec(memory_space=pltpu.VMEM)
    hbm = pl.BlockSpec(memory_space=pl.ANY)
    dma = pltpu.SemaphoreType.DMA
    small_x, small_r, small_a, all_x, all_dy, all_acts = pl.pallas_call(
        functools.partial(kernel, n_fsdp, n_ep, chunks),
        out_shape=(
            jax.ShapeDtypeStruct((n_tok, model), BF16),
            jax.ShapeDtypeStruct((EXP_WIN, n_tok), F32),
            jax.ShapeDtypeStruct(logits.shape, F32),
            jax.ShapeDtypeStruct((rows, depth), BF16),
            jax.ShapeDtypeStruct((rows, depth), BF16),
            jax.ShapeDtypeStruct((CORES, chunks, 3, rows, w), BF16),
        ),
        in_specs=[vmem] * 4 + [hbm] * 3,
        out_specs=[vmem] * 3 + [hbm] * 3,
        scratch_shapes=[
            pltpu.VMEM(w_gate.shape, BF16),
            pltpu.VMEM(w_up.shape, BF16),
            pltpu.VMEM(w_down.shape, BF16),
            pltpu.VMEM((EXP_WIN, n_fsdp, PAD, depth), BF16),
            pltpu.VMEM((n_dev, PAD, depth), BF16),
            pltpu.VMEM((rows, depth), BF16),
            pltpu.VMEM((rows, depth), BF16),
            pltpu.VMEM((items, 3, part, w), F32),
            pltpu.VMEM((items, 3, part, w), BF16),
            pltpu.VMEM((items, 3, part, w), BF16),
            pltpu.VMEM((items, 3, part, w), BF16),
            pltpu.VMEM((items, n_x - 1, 3, part, w), BF16),
            pltpu.VMEM((items, 3, part, w), BF16),
            pltpu.VMEM((items, 3, part, w), BF16),
            pltpu.VMEM((rows, depth), F32),
            pltpu.VMEM((rows, 1), F32),
            pltpu.VMEM((n_dev, PAD, depth), BF16),
            pltpu.VMEM((n_dev, PAD, depth), BF16),
            dma((3,)),
            dma((items, CORES)),
            dma((2,)),
            dma,
            dma((GROUPS,)),
            dma((items,)),
            dma((items,)),
            dma((items, n_x - 1)),
            dma((items, n_x - 1)),
            dma((items,)),
            dma((items,)),
            dma,
            dma,
        ],
        compiler_params=pltpu.CompilerParams(
            collective_id=0, has_side_effects=True, vmem_limit_bytes=62 * 1024 * 1024
        ),
    )(tokens, cotangent, jnp.transpose(routes), logits, w_gate, w_up, w_down)
    step = min(256, w)
    per = w // step

    def same(i):
        return (0, 0)

    def whole(a):
        return pl.BlockSpec(a.shape, same)

    smalls = [whole(small_x), whole(small_r), whole(small_a)]
    cols = pl.BlockSpec((depth, step), lambda i: (0, i))
    out = pl.pallas_call(
        weight_kernel,
        grid=(width // step,),
        out_shape=(
            jax.ShapeDtypeStruct(small_x.shape, BF16),
            jax.ShapeDtypeStruct(small_r.shape, F32),
            jax.ShapeDtypeStruct(small_a.shape, F32),
            jax.ShapeDtypeStruct(w_gate.shape, BF16),
            jax.ShapeDtypeStruct(w_up.shape, BF16),
            jax.ShapeDtypeStruct(w_down.shape, BF16),
        ),
        in_specs=[
            whole(all_x),
            whole(all_dy),
            pl.BlockSpec(
                (None, None, 3, rows, step),
                lambda i: (i // (chunks * per), lax.rem(i // per, chunks), 0, 0, lax.rem(i, per)),
            ),
        ]
        + smalls,
        out_specs=smalls + [cols, cols, pl.BlockSpec((step, depth), lambda i: (i, 0))],
        compiler_params=pltpu.CompilerParams(dimension_semantics=("arbitrary",)),
    )(all_x, all_dy, all_acts, small_x, small_r, small_a)
    return (out[0], jnp.transpose(out[1])) + tuple(out[2:])


def solution(mesh):
    in_specs = (
        P(("fsdp", "ep"), None),
        P(("fsdp", "ep"), None),
        P(("fsdp", "ep"), None),
        P(("fsdp", "ep"), None),
        P("fsdp", "ep"),
        P("fsdp", "ep"),
        P("ep", "fsdp"),
    )
    out_specs = (
        P(("fsdp", "ep"), None),
        P(("fsdp", "ep"), None),
        P(("fsdp", "ep"), None),
        P("fsdp", "ep"),
        P("fsdp", "ep"),
        P("ep", "fsdp"),
    )
    step = functools.partial(body, mesh.shape["fsdp"], mesh.shape["ep"])
    return jax.shard_map(step, mesh=mesh, in_specs=in_specs, out_specs=out_specs, check_vma=False)
```

```python
import functools

import jax
import jax.numpy as jnp
from jax import lax
from jax.experimental import pallas as pl
from jax.experimental.pallas import tpu as pltpu
from jax.sharding import PartitionSpec as P

EXP_WIN = 2
CAP = 3
PAD = 8
CORES = 2
CHUNKS = 4
GROUPS = 2
LAST = (((1,), (1,)), ((), ()))
FIRST = (((0,), (0,)), ((), ()))
F32 = jnp.float32
BF16 = jnp.bfloat16
MESH = pl.DeviceIdType.MESH


def iota(shape, axis):
    return lax.broadcasted_iota(jnp.int32, shape, axis)


def kernel(
    n_fsdp, n_ep, chunks,
    tok_ref, cot_ref, routes_ref, logits_ref, wg_hbm, wu_hbm, wd_hbm,
    gt_ref, rd_ref, aux_ref, x_hbm, dy_hbm, acts_hbm,
    wg, wu, wd,
    send1, recv1, rows_x, rows_dy,
    own_a, send_a, recv_a, send_b, recv_b, acts, recv_c, dx, dots, send2, recv2,
    w_sem, o_sem, x_sem, d_send, d_recv, a_send, a_recv, b_send, b_recv, c_send, c_recv, r_send, r_recv,
):
    n_dev = n_fsdp * n_ep
    n_x = n_fsdp // CORES
    blocks = n_ep // EXP_WIN
    f, e = lax.axis_index("fsdp"), lax.axis_index("ep")
    me = f * n_ep + e
    x, core = f // CORES, lax.rem(f, CORES)
    partner = x * CORES + (1 - core)
    depth, width = wg.shape
    half = width // CORES
    w = half // chunks
    ring = n_ep // GROUPS
    size = n_fsdp * ring
    span_rows = size * CAP
    place = f * ring + e // GROUPS

    def peer(t, i):
        return i // ring, lax.rem(i, ring) * GROUPS + lax.rem(e + t, GROUPS)

    barrier = pltpu.get_barrier_semaphore()

    def greet(j, _):
        d = lax.rem(me + j, n_dev)
        pl.semaphore_signal(barrier, inc=1, device_id=(d // n_ep, lax.rem(d, n_ep)), device_id_type=MESH)
        return 0

    lax.fori_loop(1, n_dev, greet, 0)
    loads = [
        pltpu.make_async_copy(s, t, w_sem.at[i])
        for i, (s, t) in enumerate(((wg_hbm, wg), (wu_hbm, wu), (wd_hbm, wd)))
    ]
    for c in loads:
        c.start()

    routes = routes_ref[...]
    logits = logits_ref[...]
    n_tok, n_exp = logits.shape
    ti, tj = iota((n_tok, n_tok), 0), iota((n_tok, n_tok), 1)
    r0, r1 = (
        jnp.sum(jnp.where(ti == tj, routes[k : k + 1, :], 0), axis=1, keepdims=True) for k in range(2)
    )
    experts = iota((n_tok, n_exp), 1)
    c0 = jnp.sum(jnp.where(experts == r0, logits, 0.0), axis=1, keepdims=True)
    c1 = jnp.sum(jnp.where(experts == r1, logits, 0.0), axis=1, keepdims=True)
    top = jnp.maximum(c0, c1)
    e0, e1 = jnp.exp(c0 - top), jnp.exp(c1 - top)
    p0, p1 = e0 / (e0 + e1), e1 / (e0 + e1)
    ci = iota((PAD, n_tok), 0)
    lanes = iota((n_tok, depth), 1)
    counts = jnp.sum(
        jnp.where(lanes == r0, 1.0, 0.0) + jnp.where(lanes == r1, 1.0, 0.0), axis=0, keepdims=True
    )
    tok = tok_ref[...]
    cot = cot_ref[...].astype(F32)
    member_col, slot_col, member_row, slot_line = [], [], [], []
    row_id = iota((PAD, depth), 0)
    for k in range(EXP_WIN):
        m0, m1 = jnp.where(r0 == k, 1.0, 0.0), jnp.where(r1 == k, 1.0, 0.0)
        col = m0 + m1
        weight = m0 * p0 + m1 * p1
        row = jnp.sum(jnp.where(ti == tj, col, 0.0), axis=0, keepdims=True)
        slot_row = jnp.sum(jnp.where(ti < tj, col, 0.0), axis=0, keepdims=True)
        slot_col.append(jnp.sum(jnp.where(tj < ti, row, 0.0), axis=1, keepdims=True))
        member_col.append(col)
        member_row.append(row)
        slot_line.append(slot_row)
        cf = ci.astype(F32)
        sel_a = jnp.where((cf == slot_row) & (ci < CAP), row, 0.0).astype(BF16)
        sel_b = jnp.where((cf - CAP == slot_row) & (ci < 2 * CAP), row, 0.0).astype(BF16)
        wcot = (cot * weight).astype(BF16)
        sent = jnp.dot(sel_a, tok, preferred_element_type=F32)
        sent = sent + jnp.dot(sel_b, wcot, preferred_element_type=F32)
        for g in range(n_fsdp):
            part = sent[:, g * depth : (g + 1) * depth]
            send1[k, g] = jnp.where(row_id == 2 * CAP, counts, part).astype(BF16)

    pl.semaphore_wait(barrier, n_dev - 1)

    recv1[place] = send1[e // blocks, f]
    for t in range(GROUPS):
        back_t = (GROUPS - t) % GROUPS

        def push(j, _, t=t, back_t=back_t):
            df, de = peer(t, lax.rem(place + j, size))
            pltpu.make_async_remote_copy(
                src_ref=send1.at[de // blocks, df], dst_ref=recv1.at[back_t * size + place],
                send_sem=d_send, recv_sem=d_recv.at[back_t], device_id=(df, de), device_id_type=MESH,
            ).start()
            return 0

        lax.fori_loop(1 if t == 0 else 0, size, push, 0)

    grp = min(16, size)
    si, sj = iota((grp * CAP, grp * PAD), 0), iota((grp * CAP, grp * PAD), 1)
    base = (si // CAP) * PAD + lax.rem(si, CAP)
    pick_x = jnp.where(sj == base, 1.0, 0.0).astype(BF16)
    pick_dy = jnp.where(sj == base + CAP, 1.0, 0.0).astype(BF16)
    pick_c = jnp.where(
        lax.rem(iota((8, grp * PAD), 1), PAD) == 2 * CAP, 1.0, 0.0
    ).astype(BF16)

    def prepare(t, total):
        landed = recv1.at[pl.ds(t * size, size - 1 if t == 0 else size)]
        pltpu.make_async_copy(landed, landed, d_recv.at[t]).wait()
        for g in range(t * size // grp, (t + 1) * size // grp):
            came = recv1[g * grp : (g + 1) * grp].reshape(grp * PAD, depth)
            span = pl.ds(g * grp * CAP, grp * CAP)
            rows_x[span] = jnp.dot(pick_x, came, preferred_element_type=F32).astype(BF16)
            rows_dy[span] = jnp.dot(pick_dy, came, preferred_element_type=F32).astype(BF16)
            total = total + jnp.dot(pick_c, came, preferred_element_type=F32)
        return total

    def copy_a(k):
        return pltpu.make_async_remote_copy(
            src_ref=send_a.at[k], dst_ref=recv_a.at[k], send_sem=a_send.at[k], recv_sem=a_recv.at[k],
            device_id=(partner, e), device_id_type=MESH,
        )

    def copy_b(k, j):
        to = lax.rem(x + j, n_x) * CORES + core
        return pltpu.make_async_remote_copy(
            src_ref=send_b.at[k], dst_ref=recv_b.at[k, j - 1], send_sem=b_send.at[k, j - 1],
            recv_sem=b_recv.at[k, j - 1], device_id=(to, e), device_id_type=MESH,
        )

    def copy_c(k):
        return pltpu.make_async_remote_copy(
            src_ref=acts.at[k], dst_ref=recv_c.at[k], send_sem=c_send.at[k], recv_sem=c_recv.at[k],
            device_id=(partner, e), device_id_type=MESH,
        )

    def columns(h, k):
        return pl.ds(pl.multiple_of(h * half + k * w, w), w)

    def group(u):
        return pl.ds(u // chunks * span_rows, span_rows)

    def partials(h, u):
        cols = columns(h, u % chunks)
        xs, dys = rows_x[group(u)], rows_dy[group(u)]
        yield jnp.dot(xs, wg[:, cols], preferred_element_type=F32)
        yield jnp.dot(xs, wu[:, cols], preferred_element_type=F32)
        yield lax.dot_general(dys, wd[cols, :], LAST, preferred_element_type=F32)

    def stage1(k):
        for i, v in enumerate(partials(1 - core, k)):
            send_a[k, i] = v.astype(BF16)
        copy_a(k).start()
        for i, v in enumerate(partials(core, k)):
            own_a[k, i] = v

    def stage2(k):
        copy_a(k).wait_recv()
        v = own_a[k] + recv_a[k].astype(F32)
        own_a[k] = v
        send_b[k] = v.astype(BF16)
        for j in range(1, n_x):
            copy_b(k, j).start()

    def stage3(k):
        for j in range(1, n_x):
            copy_b(k, j).wait_recv()
        pre = []
        for i in range(3):
            v = own_a[k, i]
            for j in range(n_x - 1):
                v = v + recv_b[k, j, i].astype(F32)
            pre.append(v)
        gate_pre, up_pre, hidden_grad = pre
        sigma = jax.nn.sigmoid(gate_pre)
        active = gate_pre * sigma
        hidden = (active * up_pre).astype(BF16)
        dot = jnp.sum(hidden.astype(F32) * hidden_grad, axis=1, keepdims=True)
        dots[group(k)] = dot if k % chunks == 0 else dots[group(k)] + dot
        acts[k, 0] = (hidden_grad * up_pre * sigma * (1.0 + gate_pre * (1.0 - sigma))).astype(BF16)
        acts[k, 1] = (hidden_grad * active).astype(BF16)
        acts[k, 2] = hidden
        copy_c(k).start()

    def grads(h, k, source):
        cols = columns(h, k % chunks)
        part = lax.dot_general(source[k, 0], wg[:, cols], LAST, preferred_element_type=F32)
        return part + lax.dot_general(source[k, 1], wu[:, cols], LAST, preferred_element_type=F32)

    def store(h, k, slot, source):
        return pltpu.make_async_copy(source.at[k], acts_hbm.at[h, k % chunks, :, group(k), :], o_sem.at[k, slot])

    row_stores = [
        pltpu.make_async_copy(rows_x, x_hbm, x_sem.at[0]),
        pltpu.make_async_copy(rows_dy, dy_hbm, x_sem.at[1]),
    ]

    def stage4(k):
        part = grads(core, k, acts)
        store(core, k, 0, acts).start()
        copy_c(k).wait_recv()
        part = part + grads(1 - core, k, recv_c)
        store(1 - core, k, 1, recv_c).start()
        dx[group(k)] = part if k % chunks == 0 else dx[group(k)] + part

    for c in loads:
        c.wait()
    total = jnp.zeros((8, depth), F32)
    for t in range(GROUPS):
        total = prepare(t, total)
        for k in range(t * chunks, (t + 1) * chunks):
            stage1(k)
            if k > 0:
                stage2(k - 1)
    stage2(GROUPS * chunks - 1)

    for c in row_stores:
        c.start()

    count = total[0:1, 0:n_exp]
    target = n_exp * (count / jnp.sum(count, axis=1, keepdims=True))
    raised = jnp.exp(logits - jnp.max(logits, axis=1, keepdims=True))
    probs = raised / jnp.sum(raised, axis=1, keepdims=True)
    aux_ref[...] = probs * (target - jnp.sum(probs * target, axis=1, keepdims=True))

    bi, bj = iota((grp * PAD, grp * CAP), 0), iota((grp * PAD, grp * CAP), 1)
    base = (bj // CAP) * PAD + lax.rem(bj, CAP)
    put_x = jnp.where(bi == base, 1.0, 0.0).astype(BF16)
    put_dot = jnp.where(bi == base + CAP, 1.0, 0.0).astype(BF16)
    once = jnp.where(x == 0, 1.0, 0.0)

    def give_back(t):
        for g in range(t * size // grp, (t + 1) * size // grp):
            span = pl.ds(g * grp * CAP, grp * CAP)
            mine = jnp.broadcast_to(dots[span] * once, (grp * CAP, depth)).astype(BF16)
            back = jnp.dot(put_x, dx[span].astype(BF16), preferred_element_type=F32)
            back = back + jnp.dot(put_dot, mine, preferred_element_type=F32)
            send2[g * grp : (g + 1) * grp] = back.astype(BF16).reshape(grp, PAD, depth)

        def give(j, _):
            i = lax.rem(place + j, size)
            pltpu.make_async_remote_copy(
                src_ref=send2.at[t * size + i], dst_ref=recv2.at[me], send_sem=r_send, recv_sem=r_recv,
                device_id=peer(t, i), device_id_type=MESH,
            ).start()
            return 0

        lax.fori_loop(1 if t == 0 else 0, size, give, 0)
        if t == 0:
            recv2[me] = send2[place]

    for k in range(GROUPS * chunks):
        stage3(k)
        if k > 0:
            stage4(k - 1)
            if k % chunks == 0:
                give_back(k // chunks - 1)
    stage4(GROUPS * chunks - 1)
    give_back(GROUPS - 1)
    everyone = recv1.at[pl.ds(0, n_dev - 1)]
    everyone2 = recv2.at[pl.ds(0, n_dev - 1)]
    pltpu.make_async_copy(everyone2, everyone2, r_recv).wait()

    route = [jnp.zeros((1, 1), F32) for _ in range(EXP_WIN * CAP)]
    for g in range(n_fsdp):
        grad = jnp.zeros((n_tok, depth), F32)
        for k in range(EXP_WIN):
            acc = recv2[g * n_ep + k * blocks].astype(F32)
            for b in range(1, blocks):
                acc = acc + recv2[g * n_ep + k * blocks + b].astype(F32)
            for c in range(CAP):
                pick = jnp.where(slot_col[k] == c, member_col[k], 0.0)
                grad = grad + pick * acc[c : c + 1, :]
                route[k * CAP + c] = route[k * CAP + c] + acc[CAP + c : CAP + c + 1, 0:1]
        gt_ref[:, g * depth : (g + 1) * depth] = grad.astype(BF16)
    which = iota((EXP_WIN, n_tok), 0)
    out = jnp.zeros((EXP_WIN, n_tok), F32)
    for k in range(EXP_WIN):
        for c in range(CAP):
            pick = jnp.where(slot_line[k] == c, member_row[k], 0.0)
            out = out + jnp.where(which == k, pick * route[k * CAP + c], 0.0)
    rd_ref[...] = out

    pltpu.make_async_copy(everyone, everyone, d_send).wait()
    pltpu.make_async_copy(everyone2, everyone2, r_send).wait()
    for k in range(GROUPS * chunks):
        copy_a(k).wait_send()
        copy_c(k).wait_send()
        for j in range(1, n_x):
            copy_b(k, j).wait_send()
        store(core, k, 0, acts).wait()
        store(1 - core, k, 1, recv_c).wait()
    for c in row_stores:
        c.wait()


def weight_kernel(x_ref, dy_ref, acts_ref, gt_in, rd_in, aux_in, gt_ref, rd_ref, aux_ref, og, ou, od):
    xs, dys = x_ref[...], dy_ref[...]
    for p in range(acts_ref.shape[0]):
        w = acts_ref.shape[3]
        c = pl.ds(p * w, w)
        og[:, c] = lax.dot_general(xs, acts_ref[p, 0], FIRST, preferred_element_type=F32).astype(BF16)
        ou[:, c] = lax.dot_general(xs, acts_ref[p, 1], FIRST, preferred_element_type=F32).astype(BF16)
        od[c, :] = lax.dot_general(acts_ref[p, 2], dys, FIRST, preferred_element_type=F32).astype(BF16)

    @pl.when(pl.program_id(0) == 0)
    def _():
        gt_ref[...] = gt_in[...]
        rd_ref[...] = rd_in[...]
        aux_ref[...] = aux_in[...]


def body(n_fsdp, n_ep, tokens, cotangent, routes, logits, w_gate, w_up, w_down):
    n_tok, model = tokens.shape
    depth, width = w_gate.shape
    n_dev = n_fsdp * n_ep
    n_x = n_fsdp // CORES
    rows = n_dev * CAP
    half = width // CORES
    chunks = max(1, min(CHUNKS, half // 128))
    w = half // chunks
    items, part = GROUPS * chunks, rows // GROUPS
    vmem = pl.BlockSpec(memory_space=pltpu.VMEM)
    hbm = pl.BlockSpec(memory_space=pl.ANY)
    dma = pltpu.SemaphoreType.DMA
    small_x, small_r, small_a, all_x, all_dy, all_acts = pl.pallas_call(
        functools.partial(kernel, n_fsdp, n_ep, chunks),
        out_shape=(
            jax.ShapeDtypeStruct((n_tok, model), BF16),
            jax.ShapeDtypeStruct((EXP_WIN, n_tok), F32),
            jax.ShapeDtypeStruct(logits.shape, F32),
            jax.ShapeDtypeStruct((rows, depth), BF16),
            jax.ShapeDtypeStruct((rows, depth), BF16),
            jax.ShapeDtypeStruct((CORES, chunks, 3, rows, w), BF16),
        ),
        in_specs=[vmem] * 4 + [hbm] * 3,
        out_specs=[vmem] * 3 + [hbm] * 3,
        scratch_shapes=[
            pltpu.VMEM(w_gate.shape, BF16),
            pltpu.VMEM(w_up.shape, BF16),
            pltpu.VMEM(w_down.shape, BF16),
            pltpu.VMEM((EXP_WIN, n_fsdp, PAD, depth), BF16),
            pltpu.VMEM((n_dev, PAD, depth), BF16),
            pltpu.VMEM((rows, depth), BF16),
            pltpu.VMEM((rows, depth), BF16),
            pltpu.VMEM((items, 3, part, w), F32),
            pltpu.VMEM((items, 3, part, w), BF16),
            pltpu.VMEM((items, 3, part, w), BF16),
            pltpu.VMEM((items, 3, part, w), BF16),
            pltpu.VMEM((items, n_x - 1, 3, part, w), BF16),
            pltpu.VMEM((items, 3, part, w), BF16),
            pltpu.VMEM((items, 3, part, w), BF16),
            pltpu.VMEM((rows, depth), F32),
            pltpu.VMEM((rows, 1), F32),
            pltpu.VMEM((n_dev, PAD, depth), BF16),
            pltpu.VMEM((n_dev, PAD, depth), BF16),
            dma((3,)),
            dma((items, CORES)),
            dma((2,)),
            dma,
            dma((GROUPS,)),
            dma((items,)),
            dma((items,)),
            dma((items, n_x - 1)),
            dma((items, n_x - 1)),
            dma((items,)),
            dma((items,)),
            dma,
            dma,
        ],
        compiler_params=pltpu.CompilerParams(
            collective_id=0, has_side_effects=True, vmem_limit_bytes=62 * 1024 * 1024
        ),
    )(tokens, cotangent, jnp.transpose(routes), logits, w_gate, w_up, w_down)
    pair = 2 if chunks % 2 == 0 else 1
    step = w * pair
    per = chunks // pair

    def same(i):
        return (0, 0)

    def whole(a):
        return pl.BlockSpec(a.shape, same)

    smalls = [whole(small_x), whole(small_r), whole(small_a)]
    cols = pl.BlockSpec((depth, step), lambda i: (0, i))
    out = pl.pallas_call(
        weight_kernel,
        grid=(width // step,),
        out_shape=(
            jax.ShapeDtypeStruct(small_x.shape, BF16),
            jax.ShapeDtypeStruct(small_r.shape, F32),
            jax.ShapeDtypeStruct(small_a.shape, F32),
            jax.ShapeDtypeStruct(w_gate.shape, BF16),
            jax.ShapeDtypeStruct(w_up.shape, BF16),
            jax.ShapeDtypeStruct(w_down.shape, BF16),
        ),
        in_specs=[
            whole(all_x),
            whole(all_dy),
            pl.BlockSpec(
                (None, pair, 3, rows, w),
                lambda i: (i // per, lax.rem(i, per), 0, 0, 0),
            ),
        ]
        + smalls,
        out_specs=smalls + [cols, cols, pl.BlockSpec((step, depth), lambda i: (i, 0))],
        compiler_params=pltpu.CompilerParams(dimension_semantics=("arbitrary",)),
    )(all_x, all_dy, all_acts, small_x, small_r, small_a)
    return (out[0], jnp.transpose(out[1])) + tuple(out[2:])


def solution(mesh):
    in_specs = (
        P(("fsdp", "ep"), None),
        P(("fsdp", "ep"), None),
        P(("fsdp", "ep"), None),
        P(("fsdp", "ep"), None),
        P("fsdp", "ep"),
        P("fsdp", "ep"),
        P("ep", "fsdp"),
    )
    out_specs = (
        P(("fsdp", "ep"), None),
        P(("fsdp", "ep"), None),
        P(("fsdp", "ep"), None),
        P("fsdp", "ep"),
        P("fsdp", "ep"),
        P("ep", "fsdp"),
    )
    step = functools.partial(body, mesh.shape["fsdp"], mesh.shape["ep"])
    return jax.shard_map(step, mesh=mesh, in_specs=in_specs, out_specs=out_specs, check_vma=False)
```
